32 devices in a mesh: tile: 16 (over z, y, core), cam: 2 (over x).
Axes of the slice: x: 2, y: 2, z: 4, core: 2. Of those that a mesh axis runs over, the one named last changes fastest.
Arguments:
- features: bfloat16 [6144, 256], P(('tile', 'cam')), may hold values from -6 to 6
- value_weight: bfloat16 [256, 256], replicated, may hold values from -0.375 to 0.375
- output_weight: bfloat16 [256, 256], replicated, may hold values from -0.375 to 0.375
- hit_list: int32 [16, 2], P('tile'), may hold values from 0 to 5, as said below
- sample_index: int32 [8192, 2, 64], P('tile'), may hold values from 0 to 1023, as said below
- attention: bfloat16 [8192, 64], P('tile'), may hold values from 0.0099487305 to 1
- validity: int32 [8192, 2], P('tile'), may hold values from 0 to 1, as said below
Outputs:
- projected: bfloat16 [8192, 256], P(('tile', 'cam'))
The draws below stay inside these ranges and needn't reach their ends.
Inputs may be any that keep to these rules, and one draw needn't show every extreme that they name: `hit_list`: camera numbers 0 to 5; where a tile sees one camera its two entries are equal. `validity`: where a tile's two hit_list entries are equal, the second column is 0 for every query of that tile. `sample_index`: for one query, slot and head, the 8 entries h * 8 to h * 8 + 7 all differ.
All inputs are finite; a program needn't handle non-finite values.
Results may differ from the reference program's by a relative error of at most 0.0058.
Values may be sent and summed in bfloat16 or wider, within the bound.
A program may use at most 64 MiB of HBM per device.

```python
import math
import jax
import jax.numpy as jnp
from jax import lax

D = 256
H = 8
K = 8
HITS = 2
CAMS = 6
CAM_ROWS = 1024
Q_TILE = 512
TILES = 16
QUERIES = 8192
FEATURE_ROWS = 6144


def camera_pairs(key):
    base_key = jax.random.fold_in(key, 7)
    lead_key, stride_key, lone_key = jax.random.split(base_key, 3)
    leading = jax.random.randint(lead_key, (TILES,), 0, CAMS)
    stride = jax.random.randint(stride_key, (TILES,), 1, CAMS)
    lonely = jax.random.randint(lone_key, (TILES,), 0, 3) == 0
    partner = jnp.where(lonely, leading, (leading + stride) % CAMS)
    return jnp.stack([leading, partner], axis=1).astype(jnp.int32)


def draw_hit_list(key, part):
    return camera_pairs(key)


def draw_validity(key, part):
    pairs = camera_pairs(key)
    query_cams = jnp.repeat(pairs, Q_TILE, axis=0)
    first_key, second_key = jax.random.split(jax.random.fold_in(key, 19))
    leading_live = jax.random.randint(first_key, (QUERIES,), 0, 5) != 0
    second_live = jax.random.randint(second_key, (QUERIES,), 0, 5) < 3
    second_live = second_live & (query_cams[:, 1] != query_cams[:, 0])
    return jnp.stack([leading_live, second_live], axis=1).astype(jnp.int32)


def draw_sample_index(key, part):
    center_key, jitter_key = jax.random.split(jax.random.fold_in(key, 31))
    spacing = CAM_ROWS // K
    center = jax.random.randint(center_key, (QUERIES, HITS, H, 1), 0, CAM_ROWS)
    jitter = jax.random.randint(jitter_key, (QUERIES, HITS, H, K), 0, spacing)
    strides = jnp.arange(K).reshape(1, 1, 1, K) * spacing
    return ((center + strides + jitter) % CAM_ROWS).reshape(QUERIES, HITS, H * K).astype(jnp.int32)


def shard_levels(key, extent, pieces, smallest, high):
    loudness = 1.0
    for dim, blocks in pieces:
        steps = jax.random.uniform(jax.random.fold_in(jax.random.fold_in(key, 6), dim), (blocks,), jnp.float32, smallest / len(pieces), high / len(pieces))
        loudness = loudness * jnp.repeat(jnp.exp(steps), extent[dim] // blocks).reshape((-1,) + (1,) * (len(extent) - 1 - dim))
    return loudness


def normal_values(rng, extent, width, limit, shards=(), kind=jnp.bfloat16):
    entries = width * jax.random.normal(rng, extent, jnp.float32)
    if shards:
        entries = entries * shard_levels(rng, extent, shards, -0.22, 0.18)
    return jnp.clip(entries, -limit, limit).astype(kind)


def setup_inputs(seed: int = 0) -> dict:
    arg_keys = jax.random.split(jax.random.key(seed), 8)
    return {
        "features": normal_values(arg_keys[0], (FEATURE_ROWS, D), 1.0, 6.0, ((0, 32),)),
        "value_weight": normal_values(arg_keys[1], (D, D), D ** -0.5, 0.375),
        "output_weight": normal_values(arg_keys[2], (D, D), D ** -0.5, 0.375),
        "hit_list": draw_hit_list(jax.random.fold_in(arg_keys[7], 71), 0),
        "sample_index": draw_sample_index(jax.random.fold_in(arg_keys[7], 71), 0),
        "attention": jnp.clip(jnp.exp(math.log(1.0) - 4.61031033 * jax.random.uniform(arg_keys[5], (QUERIES, H * K), jnp.float32) ** shard_levels(arg_keys[5], (QUERIES, H * K), ((0, 16),), -0.2, 0.2)), 0.0099487305, 1.0).astype(jnp.bfloat16),
        "validity": draw_validity(jax.random.fold_in(arg_keys[7], 71), 0),
    }


def reference(features, value_weight, output_weight, hit_list, sample_index, attention, validity):
    values = jnp.dot(features, value_weight, preferred_element_type=jnp.float32).astype(jnp.bfloat16)
    value_heads = values.astype(jnp.float32).reshape(-1, H, D // H)
    hit_count = jnp.sum(validity, axis=1)
    inverse = 1.0 / jnp.maximum(hit_count, 1).astype(jnp.float32)
    weights = attention.astype(jnp.float32).reshape(-1, 1, H, K) * validity.astype(jnp.float32)[:, :, None, None]
    weights = weights * inverse[:, None, None, None]
    cameras = jnp.repeat(hit_list, Q_TILE, axis=0).astype(jnp.int32)
    targets = (cameras[:, :, None] * CAM_ROWS + sample_index).astype(jnp.int32)
    targets = targets.reshape(TILES, Q_TILE, HITS, H, K)
    weights = weights.reshape(TILES, Q_TILE, HITS, H, K)
    head_ids = jnp.arange(H).astype(jnp.int32).reshape(1, 1, H, 1)

    def per_tile(tile_pair):
        tile_targets, tile_weights = tile_pair
        picked = value_heads[tile_targets, head_ids]
        return jnp.sum(tile_weights[..., None] * picked, axis=(1, 3))

    sampled = lax.map(per_tile, (targets, weights)).reshape(TILES * Q_TILE, D)
    attended = sampled.astype(jnp.bfloat16)
    return jnp.dot(attended, output_weight, preferred_element_type=jnp.float32).astype(jnp.bfloat16)
```

```python
import functools

import jax
import jax.numpy as jnp
from jax import lax
from jax.experimental import pallas as pl
from jax.experimental.pallas import tpu as pltpu
from jax.sharding import PartitionSpec as P

H = 8
K = 8
HITS = 2
CAMS = 6
CAM_ROWS = 1024
LANES = 128
PACK = 16
MESH = pl.DeviceIdType.MESH


class Plan:
    def __init__(self, tiles, rows, queries, width):
        self.tiles, self.rows, self.queries, self.width = tiles, rows, queries, width
        self.depth = tiles // 4
        self.chunks = 4
        self.piece = rows // self.chunks
        self.total = tiles * rows
        firsts = [[self.first(c * CAM_ROWS, x) for c in range(CAMS + 1)] for x in (0, 1)]
        extent = max(f[c + 1] - f[c] for f in firsts for c in range(CAMS))
        self.span = -(-extent // PACK) * PACK
        self.starts = [[min(f[c], self.total - self.span) for c in range(CAMS)] for f in firsts]
        self.shift = 20
        self.factor = -(-(1 << self.shift) // rows)

    def first(self, row, x):
        pair = 2 * self.rows
        return row // pair * self.rows + min(max(row % pair - x * self.rows, 0), self.rows)

    def fits(self):
        everything = CAMS * CAM_ROWS
        return (
            2 * self.total == everything
            and self.rows % (self.chunks * PACK) == 0
            and all(s % PACK == 0 for f in self.starts for s in f)
            and everything * self.factor < 1 << 31
            and all((r * self.factor) >> self.shift == r // self.rows for r in range(everything))
            and self.queries % (2 * LANES) == 0
            and self.width == 2 * LANES
        )


def fused_kernel(
    plan, hit_ref, feat_hbm, wv_hbm, wo_hbm, idx_hbm, attn_hbm, valid_hbm, out_ref,
    G, wv, wo, wvt, idx, attn, valid, weights, table, cells, vt, kept, outgoing, incoming,
    local, recv, sup, sdown, sy, sc, sx, rx,
):
    me = lax.axis_index("tile")
    x = lax.axis_index("cam")
    core = lax.rem(me, 2)
    y = lax.rem(me // 2, 2)
    z = me // 4
    depth, chunks, piece, rows = plan.depth, plan.chunks, plan.piece, plan.rows
    span, queries, width = plan.span, plan.queries, plan.width
    head_width = width // H
    share = queries // 2

    def place(zz, yy, cc):
        return (zz * 2 + yy) * 2 + cc

    def part(blk, j):
        return pl.ds(pl.multiple_of(blk * rows + j * piece, PACK), piece)

    own = place(z, y, core)
    load_feat = pltpu.make_async_copy(
        feat_hbm, G.at[pl.ds(pl.multiple_of(own * rows, PACK), rows)], local.at[0]
    )
    load_feat.start()
    loads = [
        pltpu.make_async_copy(src, dst, local.at[i + 1])
        for i, (src, dst) in enumerate(
            ((idx_hbm, idx), (attn_hbm, attn), (valid_hbm, valid), (wv_hbm, wv), (wo_hbm, wo))
        )
    ]
    for load in loads:
        load.start()

    has_up = z < depth - 1
    has_down = z > 0
    x_peer = (me, 1 - x)
    y_peer = (place(z, 1 - y, core), x)
    c_peer = (place(z, y, 1 - core), x)
    up_peer = (place(jnp.minimum(z + 1, depth - 1), y, core), x)
    down_peer = (place(jnp.maximum(z - 1, 0), y, core), x)

    barrier = pltpu.get_barrier_semaphore()
    for peer in (x_peer, y_peer, c_peer):
        pl.semaphore_signal(barrier, inc=1, device_id=peer, device_id_type=MESH)
    peers = 3
    for exists, peer in ((has_up, up_peer), (has_down, down_peer)):
        peers = peers + exists.astype(jnp.int32)

        @pl.when(exists)
        def _(peer=peer):
            pl.semaphore_signal(barrier, inc=1, device_id=peer, device_id_type=MESH)

    pl.semaphore_wait(barrier, peers)

    def copy(blk, j, send, peer):
        ref = G.at[part(blk, j)]
        return pltpu.make_async_remote_copy(
            src_ref=ref,
            dst_ref=ref,
            send_sem=send,
            recv_sem=recv.at[blk * chunks + j],
            device_id=peer,
            device_id_type=MESH,
        )

    def arrived(blk, j):
        copy(blk, j, sy.at[0], x_peer).wait_recv()

    def send_up(zz, j):
        @pl.when(has_up)
        def _():
            copy(place(zz, y, core), j, sup.at[zz * chunks + j], up_peer).start()

    def send_down(zz, j):
        @pl.when(has_down)
        def _():
            copy(place(zz, y, core), j, sdown.at[zz * chunks + j], down_peer).start()

    def send_y(zz, j):
        copy(place(zz, y, core), j, sy.at[zz * chunks + j], y_peer).start()

    def send_c(zz, across, j):
        yy = 1 - y if across else y
        slot = (zz * 2 + across) * chunks + j
        copy(place(zz, yy, core), j, sc.at[slot], c_peer).start()

    load_feat.wait()
    for j in range(chunks):
        send_up(z, j)
        send_down(z, j)
        send_y(z, j)
    for j in range(chunks):
        send_c(z, 0, j)

    for load in loads:
        load.wait()
    wvt[...] = wv[...].T
    count = jnp.maximum(jnp.sum(valid[...], axis=0, keepdims=True), 1)
    factor = valid[...].astype(jnp.float32) * (1.0 / count.astype(jnp.float32))
    scores = attn[...].astype(jnp.float32)
    starts = [jnp.where(x == 0, plan.starts[0][c], plan.starts[1][c]) for c in range(CAMS)]
    for s in range(HITS):
        hit = jnp.full((1, queries), hit_ref[0, s], jnp.int32)
        start = jnp.full((1, queries), starts[0], jnp.int32)
        for c in range(1, CAMS):
            start = jnp.where(hit == c, starts[c], start)
        points = slice(s * H * K, (s + 1) * H * K)
        row = idx[points, :] + hit * CAM_ROWS
        blk = (row * plan.factor) >> plan.shift
        near = (blk >> 1) * rows + row - blk * rows - start
        idx[points, :] = jnp.where((blk & 1) == x, near, -1)
        weights[points, :] = scores * factor[s : s + 1]

    blocks = queries // LANES
    units = H * HITS * blocks

    def unit(u, _):
        h = u // (HITS * blocks)
        s = lax.rem(u // blocks, HITS)
        lanes = pl.ds(pl.multiple_of(lax.rem(u, blocks) * LANES, LANES), LANES)
        points = pl.ds(pl.multiple_of(s * H * K + h * K, K), K)
        at = idx[points, lanes]
        wt = weights[points, lanes]
        ats = [jnp.broadcast_to(at[k : k + 1], (PACK, LANES)).astype(jnp.int16) for k in range(K)]
        wts = [jnp.broadcast_to(wt[k : k + 1], (PACK, LANES)).astype(jnp.bfloat16) for k in range(K)]
        lane_row = lax.broadcasted_iota(jnp.int32, (PACK, LANES), 0).astype(jnp.int16)
        for j in range(span // PACK):
            here = lane_row + jnp.int16(j * PACK)
            cell = jnp.zeros((PACK, LANES), jnp.bfloat16)
            for k in range(K):
                cell = jnp.where(ats[k] == here, wts[k], cell)
            first = pl.multiple_of((h * HITS + s) * span + j * PACK, PACK)
            table[pl.ds(first, PACK), lanes] = cell
        return 0

    done = [0]

    def build(count):
        count = min(count, units - done[0])
        if count > 0:
            lax.fori_loop(done[0], done[0] + count, unit, 0)
            done[0] += count

    FIRST, STEP = plan.pace
    build(FIRST)
    for wave in range(1, depth + 1):
        for j in range(chunks):
            for sign in (1, -1):
                if wave < depth:
                    zz = z - sign * wave
                    live = (zz >= 0) & (zz < depth)

                    @pl.when(live)
                    def _(zz=zz, sign=sign, j=j):
                        arrived(place(zz, y, core), j)
                        (send_up if sign > 0 else send_down)(zz, j)
                        send_y(zz, j)
                        send_c(zz, 0, j)

            for sign in (1, -1) if wave > 1 else (0,):
                zz = z - sign * (wave - 1)
                live = (zz >= 0) & (zz < depth)

                def go(zz=zz, j=j):
                    arrived(place(zz, 1 - y, core), j)
                    send_c(zz, 1, j)

                if wave > 1:
                    pl.when(live)(go)
                else:
                    go()
            build(STEP)
    build(units)

    for zz in range(depth):
        for yy in (0, 1):
            for j in range(chunks):
                arrived(place(zz, yy, 1 - core), j)

    picks = []
    for s in range(HITS):
        hit = jnp.full((PACK, width), hit_ref[0, s], jnp.int32)
        picks.append([(hit == c).astype(jnp.float32).astype(jnp.bfloat16) for c in range(CAMS)])
    for j in range(span // PACK):
        found = [jnp.zeros((PACK, width), jnp.bfloat16)] * HITS
        for c in range(CAMS):
            block = G[pl.ds(pl.multiple_of(starts[c] + j * PACK, PACK), PACK), :]
            found = [found[s] + block * picks[s][c] for s in range(HITS)]
        for s in range(HITS):
            cells[s * span + j * PACK : s * span + (j + 1) * PACK, :] = found[s]
    vt[...] = lax.dot_general(
        wvt[...], cells[...], (((1,), (1,)), ((), ())), preferred_element_type=jnp.float32
    ).astype(jnp.bfloat16)

    def sampled(h, half):
        lanes = pl.ds(pl.multiple_of(half * share, share), share)
        block = table[h * HITS * span : (h + 1) * HITS * span, lanes]
        return jnp.dot(
            vt[h * head_width : (h + 1) * head_width, :], block, preferred_element_type=jnp.float32
        )

    group = 2

    def cross(i):
        rows_i = pl.ds(i * group * head_width, group * head_width)
        return pltpu.make_async_remote_copy(
            src_ref=outgoing.at[rows_i],
            dst_ref=incoming.at[rows_i],
            send_sem=sx.at[i],
            recv_sem=rx.at[i],
            device_id=x_peer,
            device_id_type=MESH,
        )

    for h in range(H):
        outgoing[h * head_width : (h + 1) * head_width, :] = sampled(h, 1 - x).astype(jnp.bfloat16)
        if h % group == group - 1:
            cross(h // group).start()
    for h in range(H):
        kept[h * head_width : (h + 1) * head_width, :] = sampled(h, x)

    for i in range(H // group):
        cross(i).wait_recv()
    attended = (kept[...] + incoming[...].astype(jnp.float32)).astype(jnp.bfloat16)
    out_ref[...] = lax.dot_general(
        attended, wo[...], (((0,), (0,)), ((), ())), preferred_element_type=jnp.float32
    ).astype(out_ref.dtype)

    def sent(sem):
        copy(own, 0, sem, x_peer).wait_send()

    for zz in range(depth):
        for j in range(chunks):
            slot = zz * chunks + j
            pl.when(has_up & (zz <= z))(lambda slot=slot: sent(sup.at[slot]))
            pl.when(has_down & (zz >= z))(lambda slot=slot: sent(sdown.at[slot]))
            sent(sy.at[slot])
    for slot in range(depth * 2 * chunks):
        sent(sc.at[slot])
    for i in range(H // group):
        cross(i).wait_send()


def fused(plan, features, value_weight, output_weight, hit_list, index, attention, validity):
    queries, width = plan.queries, plan.width
    dma = pltpu.SemaphoreType.DMA
    points = HITS * H * K
    slots = plan.depth * plan.chunks
    bf16, f32 = jnp.bfloat16, jnp.float32
    index = index.reshape(queries, points).T
    return pl.pallas_call(
        functools.partial(fused_kernel, plan),
        out_shape=jax.ShapeDtypeStruct((queries // 2, width), bf16),
        in_specs=[pl.BlockSpec(memory_space=pltpu.SMEM)] + [pl.BlockSpec(memory_space=pl.ANY)] * 6,
        out_specs=pl.BlockSpec(memory_space=pltpu.VMEM),
        scratch_shapes=[
            pltpu.VMEM((plan.total, width), bf16),
            pltpu.VMEM((width, width), bf16),
            pltpu.VMEM((width, width), bf16),
            pltpu.VMEM((width, width), bf16),
            pltpu.VMEM((points, queries), jnp.int32),
            pltpu.VMEM((H * K, queries), bf16),
            pltpu.VMEM((HITS, queries), jnp.int32),
            pltpu.VMEM((points, queries), f32),
            pltpu.VMEM((H * HITS * plan.span, queries), bf16),
            pltpu.VMEM((HITS * plan.span, width), bf16),
            pltpu.VMEM((width, HITS * plan.span), bf16),
            pltpu.VMEM((width, queries // 2), f32),
            pltpu.VMEM((width, queries // 2), bf16),
            pltpu.VMEM((width, queries // 2), bf16),
            dma((6,)),
            dma((plan.tiles * plan.chunks,)),
            dma((slots,)),
            dma((slots,)),
            dma((slots,)),
            dma((slots * 2,)),
            dma((H // 2,)),
            dma((H // 2,)),
        ],
        compiler_params=pltpu.CompilerParams(
            collective_id=0, has_side_effects=True, vmem_limit_bytes=40 << 20
        ),
    )(hit_list, features, value_weight, output_weight, index, attention.T, validity.T)


def lane_pick(source, index):
    return jnp.take_along_axis(source, index, axis=1, mode="promise_in_bounds")


def sample_kernel(
    heads, pair, hit_ref, head_ref, vals_ref, idx_ref, attn_ref, valid_ref, out_ref, table, attns, summed
):
    width = vals_ref.shape[1]
    head_width = width // heads
    queries = idx_ref.shape[1]
    groups = queries // LANES
    parts = CAM_ROWS // LANES
    for s in range(HITS):
        for j in range(parts):
            first = pl.multiple_of(hit_ref[0, s] * CAM_ROWS + j * LANES, LANES)
            block = vals_ref[pl.ds(first, LANES), :].astype(jnp.float32)
            table[s * parts + j] = block.T
    attns[...] = attn_ref[...].astype(jnp.float32)

    def one(step, _):
        g = step * pair // heads
        lanes = pl.ds(pl.multiple_of(g * LANES, LANES), LANES)
        valid = valid_ref[:, lanes]
        count = jnp.maximum(jnp.sum(valid, axis=0, keepdims=True), 1)
        factor = valid.astype(jnp.float32) * (1.0 / count.astype(jnp.float32))
        for e in range(pair):
            h = lax.rem(step * pair, heads) + e
            attn = attns[pl.ds(pl.multiple_of((head_ref[0] + h) * K, K), K), lanes]
            acc = [jnp.zeros((8, LANES), jnp.float32)] * (head_width // 8)
            for s in range(HITS):
                index = idx_ref[pl.ds(pl.multiple_of(s * heads * K + h * K, K), K), lanes]
                low = index & (LANES - 1)
                high = index // LANES
                weight = attn * factor[s : s + 1]
                for k in range(K):
                    lo = jnp.broadcast_to(low[k : k + 1], (8, LANES))
                    hi = jnp.broadcast_to(high[k : k + 1], (8, LANES))
                    wt = jnp.broadcast_to(weight[k : k + 1], (8, LANES))
                    masks = [hi == j for j in range(parts)]
                    for d in range(head_width // 8):
                        cols = pl.ds(pl.multiple_of(h * head_width + d * 8, 8), 8)
                        picked = lane_pick(table[s * parts, cols, :], lo)
                        for j in range(1, parts):
                            got = lane_pick(table[s * parts + j, cols, :], lo)
                            picked = jnp.where(masks[j], got, picked)
                        acc[d] = acc[d] + wt * picked
            for d in range(head_width // 8):
                summed[pl.ds(pl.multiple_of(h * head_width + d * 8, 8), 8), :] = acc[d]

        @pl.when(lax.rem(step * pair, heads) == heads - pair)
        def _():
            rows = pl.ds(pl.multiple_of(g * LANES, LANES), LANES)
            out_ref[rows, :] = summed[...].T.astype(out_ref.dtype)

        return 0

    lax.fori_loop(0, groups * heads // pair, one, 0)


def sample(hit_list, vals, index, attention, validity, heads, first_head):
    queries = index.shape[0]
    width = vals.shape[1]
    padded = -(-queries // LANES) * LANES
    index = index.reshape(queries, HITS * heads * K).T
    extra = padded - queries
    index = jnp.pad(index, ((0, 0), (0, extra)))
    validity = jnp.pad(validity.T, ((0, 0), (0, extra)))
    attention = jnp.pad(attention.T, ((0, 0), (0, extra)))
    pair = 4 if heads % 4 == 0 else 1
    first_head = jnp.reshape(first_head, (1,)).astype(jnp.int32)
    out = pl.pallas_call(
        functools.partial(sample_kernel, heads, pair),
        out_shape=jax.ShapeDtypeStruct((padded, width), jnp.bfloat16),
        in_specs=[pl.BlockSpec(memory_space=pltpu.SMEM)] * 2
        + [pl.BlockSpec(memory_space=pltpu.VMEM)] * 4,
        out_specs=pl.BlockSpec(memory_space=pltpu.VMEM),
        scratch_shapes=[
            pltpu.VMEM((HITS * CAM_ROWS // LANES, width, LANES), jnp.float32),
            pltpu.VMEM(attention.shape, jnp.float32),
            pltpu.VMEM((width, LANES), jnp.float32),
        ],
    )(hit_list, first_head, vals, index, attention, validity)
    return out[:queries]


def body(features, value_weight, output_weight, hit_list, sample_index, attention, validity):
    tiles = lax.axis_size("tile")
    cams = lax.axis_size("cam")
    place = lax.axis_index("cam")
    queries = sample_index.shape[0]
    rows, width = features.shape
    if cams == 2 and tiles in (4, 8, 12, 16):
        plan = Plan(tiles, rows, queries, width)
        plan.pace = (20, 4)
        if plan.fits():
            return fused(
                plan, features, value_weight, output_weight, hit_list, sample_index, attention, validity
            )
    values = jnp.dot(features, value_weight, preferred_element_type=jnp.float32).astype(jnp.bfloat16)
    share = queries // cams
    everything = lax.all_gather(values, ("tile", "cam"), axis=0, tiled=True)
    index, weights, valid = (
        lax.dynamic_slice_in_dim(a, place * share, share, 0)
        for a in (sample_index, attention, validity)
    )
    attended = sample(hit_list, everything, index, weights, valid, H, jnp.int32(0))
    return jnp.dot(attended, output_weight, preferred_element_type=jnp.float32).astype(jnp.bfloat16)


def solution(mesh):
    in_specs = (
        P(("tile", "cam"), None),
        P(),
        P(),
        P("tile", None),
        P("tile", None, None),
        P("tile", None),
        P("tile", None),
    )
    out_specs = P(("tile", "cam"), None)
    return jax.shard_map(body, mesh=mesh, in_specs=in_specs, out_specs=out_specs, check_vma=False)
```
